16 devices in a mesh: dp: 2 (over y, z), tp: 8 (over x, core).
Axes of the slice: x: 4, y: 2, z: 1, core: 2. Of those that a mesh axis runs over, the one named last changes fastest.
The devices are a block of a 4x4x8 slice.
Arguments:
- x: bfloat16 [128, 2048], P('dp'), parts along dimension 0
- k_cache: bfloat16 [128, 4096, 8, 64], P('dp', None, 'tp'), parts along dimension 0
- v_cache: bfloat16 [128, 4096, 8, 64], P('dp', None, 'tp'), parts along dimension 0
- gain_a: bfloat16 [2048], replicated
- wq: bfloat16 [2048, 2048], P(None, 'tp')
- wo: bfloat16 [2048, 2048], P('tp')
- gain_m: bfloat16 [2048], replicated
- w_gate: bfloat16 [2048, 8192], P(None, 'tp')
- w_up: bfloat16 [2048, 8192], P(None, 'tp')
- w_down: bfloat16 [8192, 2048], P('tp')
Outputs:
- output: bfloat16 [128, 2048], P('dp'), parts along dimension 0
There are 2 independent parts. The reference program is written for one: setup_inputs(seed, part) draws one part's arguments, and reference() takes and returns one part's arrays. A program takes and returns all parts, laid end to end along the dimension named above; an argument that names none is the same for every part.
All inputs are finite; a program needn't handle non-finite values.
Results may differ from the reference program's by a relative error of at most 0.017.
Values are sent between devices in bfloat16 or wider.
A program may use at most 768 MiB of HBM per device.

```python
import jax
import jax.numpy as jnp
from jax import lax

BATCH = 64
CACHE = 4096
D = 2048
HEADS = 32
KV_HEADS = 8
HEAD = 64
FF = 8192
THETA = 10000


def setup_inputs(seed: int = 0, part: int = 0) -> dict:
    kx, kc, kw, kn, kq, ko, km, kg, ku, kd = jax.random.split(jax.random.key(seed), 10)
    kx, kc, kw = (jax.random.fold_in(k, part) for k in (kx, kc, kw))

    def weights(key, rows, columns):
        return jax.random.normal(key, (rows, columns), jnp.float32) * rows**-0.5

    drawn = {
        "x": jax.random.normal(kx, (BATCH, D), jnp.float32),
        "k_cache": 2 * jax.random.normal(kc, (BATCH, CACHE, KV_HEADS, HEAD), jnp.float32),
        "v_cache": 4 * jax.random.normal(kw, (BATCH, CACHE, KV_HEADS, HEAD), jnp.float32),
        "gain_a": 1 + 0.1 * jax.random.normal(kn, (D,), jnp.float32),
        "wq": 2 * weights(kq, D, HEADS * HEAD),
        "wo": weights(ko, HEADS * HEAD, D),
        "gain_m": 1 + 0.1 * jax.random.normal(km, (D,), jnp.float32),
        "w_gate": weights(kg, D, FF),
        "w_up": weights(ku, D, FF),
        "w_down": 2 * weights(kd, FF, D),
    }
    return {k: v.astype(jnp.bfloat16) for k, v in drawn.items()}


def normed(x, gain):
    wide = x.astype(jnp.float32)
    scale = lax.rsqrt(jnp.mean(wide * wide, -1, keepdims=True) + 1e-6)
    return (wide * scale * gain.astype(jnp.float32)).astype(jnp.bfloat16)


def turned(t, place, theta):
    half = t.shape[-1] // 2
    angle = place.astype(jnp.float32)[:, None] * theta ** (-jnp.arange(half, dtype=jnp.float32) / half)
    cos, sin = jnp.cos(angle)[:, None], jnp.sin(angle)[:, None]
    a, b = t[..., :half].astype(jnp.float32), t[..., half:].astype(jnp.float32)
    return jnp.concatenate([a * cos - b * sin, b * cos + a * sin], -1).astype(jnp.bfloat16)


def matmul(a, w):
    return jnp.dot(a, w, preferred_element_type=jnp.float32).astype(jnp.bfloat16)


def einsum(form, a, b):
    return jnp.einsum(form, a.astype(jnp.float32), b.astype(jnp.float32))


def seen_by(a, wq, k_cache, v_cache, head, theta):
    batch, cache, kv_heads = k_cache.shape[:3]
    place = jnp.full((batch,), cache - 1)
    q = turned(matmul(a, wq).reshape(batch, -1, head), place, theta).reshape(batch, kv_heads, -1, head)
    scores = einsum("bgsd,bugd->bgsu", q, k_cache) * head**-0.5
    weights = jax.nn.softmax(scores, -1).astype(jnp.bfloat16)
    return einsum("bgsu,bugd->bgsd", weights, v_cache).astype(jnp.bfloat16).reshape(batch, -1)


def hidden_of(b, w_gate, w_up):
    gate = jnp.dot(b, w_gate, preferred_element_type=jnp.float32)
    up = jnp.dot(b, w_up, preferred_element_type=jnp.float32)
    return (jax.nn.silu(gate) * up).astype(jnp.bfloat16)


def reference(x, k_cache, v_cache, gain_a, wq, wo, gain_m, w_gate, w_up, w_down):
    seen = seen_by(normed(x, gain_a), wq, k_cache, v_cache, HEAD, THETA)
    h = (x.astype(jnp.float32) + jnp.dot(seen, wo, preferred_element_type=jnp.float32)).astype(jnp.bfloat16)
    hidden = hidden_of(normed(h, gain_m), w_gate, w_up)
    return (h.astype(jnp.float32) + jnp.dot(hidden, w_down, preferred_element_type=jnp.float32)).astype(jnp.bfloat16)
```

```python
import functools

import jax
import jax.numpy as jnp
import numpy as np
from jax import lax
from jax.experimental import pallas as pl
from jax.experimental.pallas import tpu as pltpu
from jax.sharding import PartitionSpec as P

HEAD = 64
THETA = 10000
SLOTS = 8
FOUR = 4
STEP = 8
MESH = pl.DeviceIdType.MESH
ORDER = ((2, 0), (2, 1), (1, 0), (3, 0), (1, 1), (3, 1), (0, 1))
F32, BF16 = jnp.float32, jnp.bfloat16


def layer(
    chunks, x_hbm, k_hbm, v_hbm, ga_hbm, wq_hbm, wo_hbm, gm_hbm, wg_hbm, wu_hbm, wd_hbm, turn_hbm, y_hbm,
    x_ref, ga_ref, gm_ref, turn_ref, wq_ref, wo_ref, wg_ref, wu_ref, wd_ref, k_ref, v_ref, q_ref, seen_ref, a_ref, hidden_ref,
    *rest,
):
    n_chunks = len(chunks)
    own, out1, in1, h_ref, out2, in2, y_ref = (rest[i * n_chunks : (i + 1) * n_chunks] for i in range(7))
    sem, k_sem, v_sem, send_sem, recv_sem = rest[7 * n_chunks :]
    rows, d = x_ref.shape
    parts = h_ref[0].shape[0]
    part = d // parts
    groups = k_hbm.shape[0]
    me = lax.axis_index("tp")
    chip, core = me // 2, lax.rem(me, 2)

    def peer_of(ahead, other):
        return lax.rem(chip + ahead, parts // 2) * 2 + lax.rem(core + other, 2)

    def peer_from(ahead, other):
        return lax.rem(chip + parts // 2 - ahead, parts // 2) * 2 + lax.rem(core + other, 2)

    barrier = pltpu.get_barrier_semaphore()
    for ahead, other in ORDER:
        pl.semaphore_signal(barrier, inc=1, device_id={"tp": peer_of(ahead, other)}, device_id_type=MESH)

    def load(i, src, dst):
        return pltpu.make_async_copy(src, dst, sem.at[i])

    first = [load(0, x_hbm, x_ref), load(1, ga_hbm, ga_ref), load(2, turn_hbm, turn_ref), load(3, wq_hbm, wq_ref)]
    second = [load(4, wo_hbm, wo_ref), load(5, gm_hbm, gm_ref)]
    third = [load(6, wg_hbm, wg_ref), load(7, wu_hbm, wu_ref), load(8, wd_hbm, wd_ref)]

    def load_k(g, slot):
        return pltpu.make_async_copy(k_hbm.at[g], k_ref.at[slot], k_sem.at[slot])

    def load_v(g, slot):
        return pltpu.make_async_copy(v_hbm.at[g], v_ref.at[slot], v_sem.at[slot])

    for c in first:
        c.start()
    for g in range(SLOTS):
        load_k(g, g).start()
        load_v(g, g).start()
        if g == 1:
            for c in second:
                c.start()

    for c in first:
        c.wait()
    wide = x_ref[...].astype(F32)
    scale = lax.rsqrt(jnp.mean(wide * wide, -1, keepdims=True) + 1e-6)
    a = (wide * scale * ga_ref[...].astype(F32)).astype(BF16)
    q = jnp.dot(a, wq_ref[...], preferred_element_type=F32).astype(BF16).astype(F32)
    lane = lax.broadcasted_iota(jnp.int32, q.shape, 1)
    width = q.shape[1]
    swapped = jnp.where(lane % HEAD < HEAD // 2, pltpu.roll(q, width - HEAD // 2, 1), pltpu.roll(q, HEAD // 2, 1))
    q_ref[...] = (q * turn_ref[0:1, :] + swapped * turn_ref[1:2, :]).astype(BF16).astype(F32)

    lane8 = lax.broadcasted_iota(jnp.int32, (STEP, width), 1) // HEAD
    row8 = lax.broadcasted_iota(jnp.int32, (STEP, width), 0)
    low = row8 < FOUR
    zero = jnp.zeros((STEP, width), F32)

    def everywhere(t):
        t = t + pltpu.roll(t, HEAD, 1)
        return t + pltpu.roll(t, 2 * HEAD, 1)

    def spread(rep):
        halves = []
        for j in range(2):
            z = everywhere(jnp.where(lane8 == 2 * j + row8 // FOUR, rep, zero))
            halves.append(jnp.where(lane8 == row8 % FOUR, z, zero))
        return jnp.concatenate(halves, 0).astype(BF16)

    def gathered(o):
        total = zero
        for j in range(2):
            z = everywhere(jnp.where(lane8 == row8 % FOUR, o[STEP * j : STEP * (j + 1)], zero))
            total = total + jnp.where(lane8 == 2 * j + row8 // FOUR, z, zero)
        return total + pltpu.roll(total, FOUR, 0)

    def attend(i, _):
        q8 = q_ref[pl.ds(pl.multiple_of(i * STEP, STEP), STEP), :]
        turned8 = pltpu.roll(q8, FOUR, 0)
        done = []
        for half in range(2):
            g = 2 * i + half
            slot = lax.rem(g, SLOTS)
            load_k(g, slot).wait()
            load_v(g, slot).wait()
        for half in range(2):
            slot = lax.rem(2 * i + half, SLOTS)
            rep = jnp.where(low, q8, turned8) if half == 0 else jnp.where(low, turned8, q8)
            s = jnp.dot(spread(rep), k_ref[slot], preferred_element_type=F32)
            top = jnp.max(s, -1, keepdims=True)
            e = jnp.exp((s - top) * HEAD**-0.5)
            w = (e * (1.0 / jnp.sum(e, -1, keepdims=True))).astype(BF16)
            o = lax.dot_general(w, v_ref[slot], (((1,), (1,)), ((), ())), preferred_element_type=F32)
            done.append(gathered(o))
        seen_ref[pl.ds(pl.multiple_of(i * STEP, STEP), STEP), :] = jnp.where(low, done[0], done[1])
        for half in range(2):
            g = 2 * i + half

            @pl.when(g + SLOTS < groups)
            def _():
                slot = lax.rem(g, SLOTS)
                load_k(g + SLOTS, slot).start()
                load_v(g + SLOTS, slot).start()

        return 0

    def sent(c, phase, src, dst, peer):
        s = (c * 4 + phase) * parts
        return pltpu.make_async_remote_copy(
            src_ref=src, dst_ref=dst, send_sem=send_sem.at[s + peer], recv_sem=recv_sem.at[s + me], device_id={"tp": peer}, device_id_type=MESH
        )

    def got(c, phase, dst, peer):
        s = (c * 4 + phase) * parts
        pltpu.make_async_remote_copy(
            src_ref=dst, dst_ref=dst, send_sem=send_sem.at[s + peer], recv_sem=recv_sem.at[s + peer], device_id={"tp": peer}, device_id_type=MESH
        ).wait_recv()

    def cols(p):
        return pl.ds(pl.multiple_of(p * part, part), part)

    def scatter(c, phase, left, w_ref, out, into):
        for ahead, other in ORDER + ((0, 0),):
            p = peer_of(ahead, other)
            term = jnp.dot(left, w_ref[:, cols(p)], preferred_element_type=F32)
            if (ahead, other) == (0, 0):
                own[c][...] = term
            else:
                out[c][p] = term.astype(BF16)
                sent(c, phase, out[c].at[p], into[c].at[me], p).start()

    def summed(c, phase, into, residual):
        total = own[c][...]
        for ahead, other in reversed(ORDER):
            p = peer_from(ahead, other)
            got(c, phase, into[c].at[p], p)
            total = total + into[c][p].astype(F32)
        return (residual + total).astype(BF16)

    def spans(c):
        start, size = chunks[c]
        return pl.ds(start, size)

    def first_half(c):
        scatter(c, 0, seen_ref[spans(c), :].astype(BF16), wo_ref, out1, in1)

    def first_sum(c):
        h_ref[c][me] = summed(c, 0, in1, x_ref[spans(c), cols(me)].astype(F32))
        for ahead, other in ORDER:
            p = peer_of(ahead, other)
            sent(c, 1, h_ref[c].at[me], h_ref[c].at[me], p).start()

    def second_half(c):
        start, size = chunks[c]
        for ahead, other in reversed(ORDER):
            p = peer_from(ahead, other)
            got(c, 1, h_ref[c].at[p], p)
        squares = jnp.zeros((size, part), F32)
        for p in range(parts):
            wide = h_ref[c][p].astype(F32)
            squares = squares + wide * wide
        scale = lax.rsqrt(jnp.sum(squares, -1, keepdims=True) * (1.0 / d) + 1e-6)
        for p in range(parts):
            gain = gm_ref[:, p * part : (p + 1) * part].astype(F32)
            a_ref[0:size, p * part : (p + 1) * part] = (h_ref[c][p].astype(F32) * scale * gain).astype(BF16)
        tile = 256

        def unit(n, _):
            at = pl.ds(pl.multiple_of(n * tile, tile), tile)
            b = a_ref[0:size, :]
            gate = jnp.dot(b, wg_ref[:, at], preferred_element_type=F32)
            up = jnp.dot(b, wu_ref[:, at], preferred_element_type=F32)
            hidden_ref[0:size, at] = (gate * (1.0 / (1.0 + jnp.exp(-gate))) * up).astype(BF16)
            return 0

        lax.fori_loop(0, wg_ref.shape[1] // tile, unit, 0)
        scatter(c, 2, hidden_ref[0:size, :], wd_ref, out2, in2)

    def second_sum(c):
        y_ref[c][...] = summed(c, 2, in2, h_ref[c][me].astype(F32))
        at = y_hbm.at[spans(c), cols(me)]
        for ahead, other in ORDER:
            p = peer_of(ahead, other)
            sent(c, 3, y_ref[c], at, p).start()
        load(9 + c, y_ref[c], at).start()

    def last(c):
        at = y_hbm.at[spans(c), cols(me)]
        for ahead, other in reversed(ORDER):
            p = peer_from(ahead, other)
            got(c, 3, y_hbm.at[spans(c), cols(p)], p)
        load(9 + c, y_ref[c], at).wait()
        for ahead, other in ORDER:
            p = peer_of(ahead, other)
            sent(c, 0, out1[c].at[p], in1[c].at[me], p).wait_send()
            sent(c, 1, h_ref[c].at[me], h_ref[c].at[me], p).wait_send()
            sent(c, 2, out2[c].at[p], in2[c].at[me], p).wait_send()
            sent(c, 3, y_ref[c], at, p).wait_send()

    half_way = chunks[0][1] // STEP
    steps = rows // STEP
    lax.fori_loop(0, half_way, attend, 0)
    for c in second:
        c.wait()
    pl.semaphore_wait(barrier, len(ORDER))
    first_half(0)
    for c in third:
        c.start()
    lax.fori_loop(half_way, steps, attend, 0)
    first_half(1)
    first_sum(0)
    for c in third:
        c.wait()
    second_half(0)
    first_sum(1)
    second_sum(0)
    second_half(1)
    second_sum(1)
    last(0)
    last(1)


def solution(mesh):
    parts = mesh.shape["tp"]

    def step(x, k_cache, v_cache, gain_a, wq, wo, gain_m, w_gate, w_up, w_down):
        rows, d = x.shape
        seqs, places, kv_heads, head = k_cache.shape
        width = wq.shape[1]
        part = d // parts
        k, v = (jnp.transpose(t, (0, 2, 3, 1)).reshape(seqs // FOUR, FOUR * kv_heads * head, places) for t in (k_cache, v_cache))
        half = head // 2
        angle = np.float32(places - 1) * np.float32(THETA) ** (-np.arange(half, dtype=np.float32) / np.float32(half))
        angle = angle.astype(np.float32)
        cos, sin = np.cos(angle).astype(np.float32), np.sin(angle).astype(np.float32)
        turn = np.stack([np.tile(cos, width // half), np.tile(np.concatenate([-sin, sin]), width // head)])
        late = 2 * STEP
        chunks = ((0, rows - late), (rows - late, late))
        sizes = [size for _, size in chunks]
        scratch = [
            pltpu.VMEM(x.shape, BF16),
            pltpu.VMEM((1, d), BF16),
            pltpu.VMEM((1, d), BF16),
            pltpu.VMEM(turn.shape, F32),
            *[pltpu.VMEM(w.shape, BF16) for w in (wq, wo, w_gate, w_up, w_down)],
            pltpu.VMEM((SLOTS,) + k.shape[1:], BF16),
            pltpu.VMEM((SLOTS,) + v.shape[1:], BF16),
            pltpu.VMEM((rows, width), F32),
            pltpu.VMEM((rows, width), F32),
            pltpu.VMEM((max(sizes), d), BF16),
            pltpu.VMEM((max(sizes), w_gate.shape[1]), BF16),
        ]
        scratch += [pltpu.VMEM((size, part), F32) for size in sizes]
        for _ in range(5):
            scratch += [pltpu.VMEM((parts, size, part), BF16) for size in sizes]
        scratch += [pltpu.VMEM((size, part), BF16) for size in sizes]
        scratch += [
            pltpu.SemaphoreType.DMA((9 + len(chunks),)),
            pltpu.SemaphoreType.DMA((SLOTS,)),
            pltpu.SemaphoreType.DMA((SLOTS,)),
            pltpu.SemaphoreType.DMA((len(chunks) * 4 * parts,)),
            pltpu.SemaphoreType.DMA((len(chunks) * 4 * parts,)),
        ]
        return pl.pallas_call(
            functools.partial(layer, chunks),
            out_shape=jax.ShapeDtypeStruct(x.shape, BF16),
            in_specs=[pl.BlockSpec(memory_space=pl.ANY)] * 11,
            out_specs=pl.BlockSpec(memory_space=pl.ANY),
            scratch_shapes=scratch,
            compiler_params=pltpu.CompilerParams(collective_id=0, has_side_effects=True, vmem_limit_bytes=64 * 1024 * 1024 - 65536),
            name="layer",
        )(x, k, v, gain_a.reshape(1, -1), wq, wo, gain_m.reshape(1, -1), w_gate, w_up, w_down, jnp.asarray(turn))

    states, cache, columns, rows_of = P("dp", None), P("dp", None, "tp", None), P(None, "tp"), P("tp", None)
    return jax.shard_map(
        step,
        mesh=mesh,
        in_specs=(states, cache, cache, P(None), columns, rows_of, P(None), columns, columns, rows_of),
        out_specs=states,
        check_vma=False,
    )
```

```python
import functools

import jax
import jax.numpy as jnp
import numpy as np
from jax import lax
from jax.experimental import pallas as pl
from jax.experimental.pallas import tpu as pltpu
from jax.sharding import PartitionSpec as P

HEAD = 64
THETA = 10000
SLOTS = 6
AHEAD = 2
FOUR = 4
STEP = 8
MESH = pl.DeviceIdType.MESH
ORDER = ((2, 0), (2, 1), (1, 0), (3, 0), (1, 1), (3, 1), (0, 1))
HERE = ((0, 0),)
F32, BF16 = jnp.float32, jnp.bfloat16


def layer(
    chunks, x_hbm, k_hbm, v_hbm, ga_hbm, wq_hbm, wo_hbm, gm_hbm, wg_hbm, wu_hbm, wd_hbm, turn_hbm, y_ref,
    x_ref, ga_ref, gm_ref, turn_ref, wq_ref, wo_ref, wg_ref, wu_ref, wd_ref, k_ref, v_ref, w_ref, q_ref, seen_ref, a_ref, hidden_ref,
    *rest,
):
    n_chunks = len(chunks)
    own, out1, in1, h_ref, out2, in2 = (rest[i * n_chunks : (i + 1) * n_chunks] for i in range(6))
    sem, k_sem, v_sem, send_sem, recv_sem = rest[6 * n_chunks :]
    rows, d = x_ref.shape
    parts = h_ref[0].shape[0]
    part = d // parts
    groups = k_hbm.shape[0]
    me = lax.axis_index("tp")
    chip, core = me // 2, lax.rem(me, 2)

    def peer_of(ahead, other):
        return lax.rem(chip + ahead, parts // 2) * 2 + lax.rem(core + other, 2)

    def peer_from(ahead, other):
        return lax.rem(chip + parts // 2 - ahead, parts // 2) * 2 + lax.rem(core + other, 2)

    barrier = pltpu.get_barrier_semaphore()
    for ahead, other in ORDER:
        pl.semaphore_signal(barrier, inc=1, device_id={"tp": peer_of(ahead, other)}, device_id_type=MESH)

    def load(i, src, dst):
        return pltpu.make_async_copy(src, dst, sem.at[i])

    first = [load(0, x_hbm, x_ref), load(1, ga_hbm, ga_ref), load(2, turn_hbm, turn_ref), load(3, wq_hbm, wq_ref)]
    second = [load(4, wo_hbm, wo_ref), load(5, gm_hbm, gm_ref)]
    third = [load(6, wg_hbm, wg_ref), load(7, wu_hbm, wu_ref), load(8, wd_hbm, wd_ref)]

    def load_k(g):
        slot = lax.rem(g, SLOTS)
        return pltpu.make_async_copy(k_hbm.at[g], k_ref.at[slot], k_sem.at[slot])

    def load_v(g):
        slot = lax.rem(g, SLOTS)
        return pltpu.make_async_copy(v_hbm.at[g], v_ref.at[slot], v_sem.at[slot])

    for c in first:
        c.start()
    for c in (load_k(0), load_k(1), load_v(0)):
        c.start()

    with jax.named_scope("wait_x"):
        for c in first:
            c.wait()
    load_v(1).start()
    for g in range(2, 2 * AHEAD):
        load_k(g).start()
        load_v(g).start()
    for c in second:
        c.start()
    wide = x_ref[...].astype(F32)
    scale = lax.rsqrt(jnp.mean(wide * wide, -1, keepdims=True) + 1e-6)
    a = (wide * scale * ga_ref[...].astype(F32).reshape(1, d)).astype(BF16)
    q = jnp.dot(a, wq_ref[...], preferred_element_type=F32).astype(BF16).astype(F32)
    lane = lax.broadcasted_iota(jnp.int32, q.shape, 1)
    width = q.shape[1]
    swapped = jnp.where(lane % HEAD < HEAD // 2, pltpu.roll(q, width - HEAD // 2, 1), pltpu.roll(q, HEAD // 2, 1))
    q_ref[...] = (q * turn_ref[0:1, :] + swapped * turn_ref[1:2, :]).astype(BF16).astype(F32)

    lane8 = lax.broadcasted_iota(jnp.int32, (STEP, width), 1) // HEAD
    row8 = lax.broadcasted_iota(jnp.int32, (STEP, width), 0)
    low = row8 < FOUR
    zero = jnp.zeros((STEP, width), F32)

    def everywhere(t):
        t = t + pltpu.roll(t, HEAD, 1)
        return t + pltpu.roll(t, 2 * HEAD, 1)

    def spread(rep):
        halves = []
        for j in range(2):
            z = everywhere(jnp.where(lane8 == 2 * j + row8 // FOUR, rep, zero))
            halves.append(jnp.where(lane8 == row8 % FOUR, z, zero))
        return jnp.concatenate(halves, 0).astype(BF16)

    def gathered(o):
        total = zero
        for j in range(2):
            z = everywhere(jnp.where(lane8 == row8 % FOUR, o[STEP * j : STEP * (j + 1)], zero))
            total = total + jnp.where(lane8 == 2 * j + row8 // FOUR, z, zero)
        return total + pltpu.roll(total, FOUR, 0)

    def scores(i, half, q8):
        turned8 = pltpu.roll(q8, FOUR, 0)
        rep = jnp.where(low, q8, turned8) if half == 0 else jnp.where(low, turned8, q8)
        s = jnp.dot(spread(rep), k_ref[lax.rem(2 * i + half, SLOTS)], preferred_element_type=F32)
        top = jnp.max(s, -1, keepdims=True)
        e = jnp.exp((s - top) * HEAD**-0.5)
        return (e * (1.0 / jnp.sum(e, -1, keepdims=True))).astype(BF16)

    def values(i, half, w):
        v = v_ref[lax.rem(2 * i + half, SLOTS)]
        return gathered(lax.dot_general(w, v, (((1,), (1,)), ((), ())), preferred_element_type=F32))

    def eight(i):
        return pl.ds(pl.multiple_of(i * STEP, STEP), STEP)

    def ahead_of(i):
        for half in range(2):
            g = 2 * (i + AHEAD) + half

            @pl.when(g < groups)
            def _():
                load_k(g).start()
                load_v(g).start()

    def wait_k(i):
        with jax.named_scope("wait_k"):
            for half in range(2):
                load_k(2 * i + half).wait()

    def wait_v(i):
        with jax.named_scope("wait_v"):
            for half in range(2):
                load_v(2 * i + half).wait()

    def attend(i, _):
        ahead_of(i)
        wait_k(i)
        wait_v(i)
        q8 = q_ref[eight(i), :]
        done = [values(i, half, scores(i, half, q8)) for half in range(2)]
        seen_ref[eight(i), :] = jnp.where(low, done[0], done[1])
        return 0

    def attend_weights(i):
        ahead_of(i)
        wait_k(i)
        q8 = q_ref[eight(i), :]
        for half in range(2):
            w_ref[half] = scores(i, half, q8)

    def attend_values(i):
        wait_v(i)
        seen_ref[eight(i), :] = jnp.where(low, values(i, 0, w_ref[0]), values(i, 1, w_ref[1]))

    def sent(c, phase, src, dst, peer):
        s = (c * 4 + phase) * parts
        return pltpu.make_async_remote_copy(
            src_ref=src, dst_ref=dst, send_sem=send_sem.at[s + peer], recv_sem=recv_sem.at[s + me], device_id={"tp": peer}, device_id_type=MESH
        )

    def got(c, phase, dst, peer):
        s = (c * 4 + phase) * parts
        pltpu.make_async_remote_copy(
            src_ref=dst, dst_ref=dst, send_sem=send_sem.at[s + peer], recv_sem=recv_sem.at[s + peer], device_id={"tp": peer}, device_id_type=MESH
        ).wait_recv()

    def cols(p):
        return pl.ds(pl.multiple_of(p * part, part), part)

    def scatter(c, phase, left, w_ref, out, into, sets):
        for peers in sets:
            for ahead, other in peers:
                p = peer_of(ahead, other)
                term = jnp.dot(left, w_ref[:, cols(p)], preferred_element_type=F32)
                if (ahead, other) == (0, 0):
                    own[c][...] = term
                else:
                    out[c][p] = term.astype(BF16)
            for ahead, other in peers:
                if (ahead, other) != (0, 0):
                    p = peer_of(ahead, other)
                    sent(c, phase, out[c].at[p], into[c].at[me], p).start()

    def summed(c, phase, into, residual):
        total = own[c][...]
        for ahead, other in reversed(ORDER):
            p = peer_from(ahead, other)
            got(c, phase, into[c].at[p], p)
            total = total + into[c][p].astype(F32)
        return (residual + total).astype(BF16)

    def spans(c):
        start, size, _ = chunks[c]
        return pl.ds(start, size)

    def direct(c):
        return chunks[c][2]

    chips = parts // 2
    half_d = d // 2

    def half_of(core_):
        return pl.ds(pl.multiple_of(core_ * half_d, half_d), half_d)

    def to_other(c, phase, left, w_ref, out, into):
        p = peer_of(0, 1)
        out[c][0] = jnp.dot(left, w_ref[:, half_of(1 - core)], preferred_element_type=F32).astype(BF16)
        sent(c, phase, out[c].at[0], into[c].at[parts], p).start()
        own[c][...] = jnp.dot(left, w_ref[:, half_of(core)], preferred_element_type=F32)

    def to_all(c, phase, out, into):
        got(c, phase, into[c].at[parts], peer_of(0, 1))
        both = (own[c][...] + into[c][parts].astype(F32)).astype(BF16)
        out[c][1] = both
        into[c][core * chips + chip] = both
        for ahead, other in ORDER:
            sent(c, phase + 1, out[c].at[1], into[c].at[core * chips + chip], peer_of(ahead, other)).start()

    def from_all(c, phase, into):
        for ahead, other in ORDER:
            p = peer_from(ahead, other)
            got(c, phase + 1, into[c].at[lax.rem(p, 2) * chips + p // 2], p)

    def summed_all(c, into, residual, q):
        which, at = q * part // half_d, q * part % half_d
        total = into[c][which * chips, :, at : at + part].astype(F32)
        for p in range(1, chips):
            total = total + into[c][which * chips + p, :, at : at + part].astype(F32)
        return (residual + total).astype(BF16)

    def first_half(c):
        left = seen_ref[spans(c), :].astype(BF16)
        if direct(c):
            to_other(c, 0, left, wo_ref, out1, in1)
        else:
            scatter(c, 0, left, wo_ref, out1, in1, (ORDER + HERE,))

    def first_sum(c):
        if direct(c):
            to_all(c, 0, out1, in1)
            return
        h_ref[c][me] = summed(c, 0, in1, x_ref[spans(c), cols(me)].astype(F32))
        for ahead, other in ORDER:
            p = peer_of(ahead, other)
            sent(c, 1, h_ref[c].at[me], h_ref[c].at[me], p).start()

    def normed_first(c):
        _, size, _ = chunks[c]
        if direct(c):
            from_all(c, 0, in1)
            for p in range(parts):
                h_ref[c][p] = summed_all(c, in1, x_ref[spans(c), p * part : (p + 1) * part].astype(F32), p)
        else:
            for ahead, other in reversed(ORDER):
                p = peer_from(ahead, other)
                got(c, 1, h_ref[c].at[p], p)
        squares = jnp.zeros((size, part), F32)
        for p in range(parts):
            wide = h_ref[c][p].astype(F32)
            squares = squares + wide * wide
        scale = lax.rsqrt(jnp.sum(squares, -1, keepdims=True) * (1.0 / d) + 1e-6)
        for p in range(parts):
            gain = gm_ref[p * part : (p + 1) * part].astype(F32).reshape(1, part)
            a_ref[0:size, p * part : (p + 1) * part] = (h_ref[c][p].astype(F32) * scale * gain).astype(BF16)

    def hidden(c):
        size = chunks[c][1]
        tile = 512
        b = a_ref[0:size, :]
        for n in range(0, wg_ref.shape[1], tile):
            gate = jnp.dot(b, wg_ref[:, n : n + tile], preferred_element_type=F32)
            up = jnp.dot(b, wu_ref[:, n : n + tile], preferred_element_type=F32)
            hidden_ref[0:size, n : n + tile] = (gate * (1.0 / (1.0 + jnp.exp(-gate))) * up).astype(BF16)

    def second_half(c):
        left = hidden_ref[0 : chunks[c][1], :]
        if direct(c):
            to_other(c, 2, left, wd_ref, out2, in2)
        else:
            scatter(c, 2, left, wd_ref, out2, in2, (ORDER[:4], ORDER[4:] + HERE))

    def second_sum(c):
        if direct(c):
            to_all(c, 2, out2, in2)
            return
        at = y_ref.at[spans(c), cols(me)]
        at[...] = summed(c, 2, in2, h_ref[c][me].astype(F32))
        for ahead, other in ORDER:
            sent(c, 3, at, at, peer_of(ahead, other)).start()

    def last(c):
        if direct(c):
            from_all(c, 2, in2)
            for p in range(parts):
                y_ref[spans(c), p * part : (p + 1) * part] = summed_all(c, in2, h_ref[c][p].astype(F32), p)
            return
        for ahead, other in reversed(ORDER):
            p = peer_from(ahead, other)
            got(c, 3, y_ref.at[spans(c), cols(p)], p)

    def all_sent(c):
        at = y_ref.at[spans(c), cols(me)]
        if direct(c):
            mine = core * chips + chip
            for phase, out, into in ((0, out1, in1), (2, out2, in2)):
                sent(c, phase, out[c].at[0], into[c].at[parts], peer_of(0, 1)).wait_send()
                for ahead, other in ORDER:
                    sent(c, phase + 1, out[c].at[1], into[c].at[mine], peer_of(ahead, other)).wait_send()
            return
        for ahead, other in ORDER:
            p = peer_of(ahead, other)
            sent(c, 0, out1[c].at[p], in1[c].at[me], p).wait_send()
            sent(c, 1, h_ref[c].at[me], h_ref[c].at[me], p).wait_send()
            sent(c, 2, out2[c].at[p], in2[c].at[me], p).wait_send()
            sent(c, 3, at, at, p).wait_send()

    scope = jax.named_scope
    big, mid, late = range(3)
    ends = [(start + size) // STEP for start, size, _ in chunks]
    steps = ends[late]
    attend_weights(0)
    attend_values(0)
    lax.fori_loop(1, ends[big], attend, 0)
    with scope("wait_wo"):
        for c in second:
            c.wait()
        pl.semaphore_wait(barrier, len(ORDER))
    with scope("first0"):
        first_half(big)
    lax.fori_loop(ends[big], ends[mid], attend, 0)
    for c in third:
        c.start()
    with scope("first1"):
        first_half(mid)
    with scope("sum0"):
        first_sum(big)
    attend_weights(steps - 1)
    attend_values(steps - 1)
    with scope("first2"):
        first_half(late)
    with scope("sum1"):
        first_sum(mid)
    with scope("sum2"):
        first_sum(late)
    with scope("norm0"):
        normed_first(big)
    with scope("wait_w"):
        for c in third:
            c.wait()
    with scope("hidden0"):
        hidden(big)
    with scope("second0"):
        second_half(big)
    with scope("norm1"):
        normed_first(mid)
    with scope("hidden1"):
        hidden(mid)
    with scope("second1"):
        second_half(mid)
    with scope("norm2"):
        normed_first(late)
    with scope("hidden2"):
        hidden(late)
    with scope("second2"):
        second_half(late)
    with scope("ysum0"):
        second_sum(big)
    with scope("ysum2"):
        second_sum(late)
    with scope("ysum1"):
        second_sum(mid)
    with scope("last0"):
        last(big)
    with scope("last1"):
        last(mid)
    with scope("last2"):
        last(late)
    with scope("sent"):
        for c in range(n_chunks):
            all_sent(c)


def solution(mesh):
    parts = mesh.shape["tp"]

    def step(x, k_cache, v_cache, gain_a, wq, wo, gain_m, w_gate, w_up, w_down):
        rows, d = x.shape
        seqs, places, kv_heads, head = k_cache.shape
        width = wq.shape[1]
        part = d // parts
        k, v = (jnp.transpose(t, (0, 2, 3, 1)).reshape(seqs // FOUR, FOUR * kv_heads * head, places) for t in (k_cache, v_cache))
        half = head // 2
        angle = np.float32(places - 1) * np.float32(THETA) ** (-np.arange(half, dtype=np.float32) / np.float32(half))
        angle = angle.astype(np.float32)
        cos, sin = np.cos(angle).astype(np.float32), np.sin(angle).astype(np.float32)
        turn = np.stack([np.tile(cos, width // half), np.tile(np.concatenate([-sin, sin]), width // head)])
        mid, late = 2 * STEP, STEP
        big = rows - mid - late
        chunks = ((0, big, False), (big, mid, False), (big + mid, late, True))
        sizes = [size for _, size, _ in chunks]
        scratch = [
            pltpu.VMEM(x.shape, BF16),
            pltpu.VMEM((d,), BF16),
            pltpu.VMEM((d,), BF16),
            pltpu.VMEM(turn.shape, F32),
            *[pltpu.VMEM(w.shape, BF16) for w in (wq, wo, w_gate, w_up, w_down)],
            pltpu.VMEM((SLOTS,) + k.shape[1:], BF16),
            pltpu.VMEM((SLOTS,) + v.shape[1:], BF16),
            pltpu.VMEM((2, FOUR * width // head, places), BF16),
            pltpu.VMEM((rows, width), F32),
            pltpu.VMEM((rows, width), F32),
            pltpu.VMEM((max(sizes), d), BF16),
            pltpu.VMEM((max(sizes), w_gate.shape[1]), BF16),
        ]
        scratch += [pltpu.VMEM((size, d // 2 if whole else part), F32) for _, size, whole in chunks]
        blocks = [pltpu.VMEM((parts, size, part), BF16) for size in sizes]
        outs = [pltpu.VMEM((2, size, d // 2) if whole else (parts, size, part), BF16) for _, size, whole in chunks]
        ins = [pltpu.VMEM((parts + 1, size, d // 2) if whole else (parts, size, part), BF16) for _, size, whole in chunks]
        scratch += outs + ins + blocks + outs + ins
        scratch += [
            pltpu.SemaphoreType.DMA((9,)),
            pltpu.SemaphoreType.DMA((SLOTS,)),
            pltpu.SemaphoreType.DMA((SLOTS,)),
            pltpu.SemaphoreType.DMA((len(chunks) * 4 * parts,)),
            pltpu.SemaphoreType.DMA((len(chunks) * 4 * parts,)),
        ]
        return pl.pallas_call(
            functools.partial(layer, chunks),
            out_shape=pltpu.VMEM(x.shape, BF16),
            in_specs=[pl.BlockSpec(memory_space=pl.ANY)] * 11,
            out_specs=pl.BlockSpec(memory_space=pltpu.VMEM),
            scratch_shapes=scratch,
            compiler_params=pltpu.CompilerParams(collective_id=0, has_side_effects=True, vmem_limit_bytes=60 * 1024 * 1024),
            name="layer",
        )(x, k, v, gain_a, wq, wo, gain_m, w_gate, w_up, w_down, jnp.asarray(turn))

    states, cache, columns, rows_of = P("dp", None), P("dp", None, "tp", None), P(None, "tp"), P("tp", None)
    return jax.shard_map(
        step,
        mesh=mesh,
        in_specs=(states, cache, cache, P(None), columns, rows_of, P(None), columns, columns, rows_of),
        out_specs=states,
        check_vma=False,
    )
```

```python
import functools

import jax
import jax.numpy as jnp
import numpy as np
from jax import lax
from jax.experimental import pallas as pl
from jax.experimental.pallas import tpu as pltpu
from jax.sharding import PartitionSpec as P

HEAD = 64
THETA = 10000
SLOTS = 3
DEPTH = 4
FOUR = 4
STEP = 8
MESH = pl.DeviceIdType.MESH
ORDER = ((2, 0), (2, 1), (1, 0), (3, 0), (1, 1), (3, 1), (0, 1))
HERE = ((0, 0),)
F32, BF16 = jnp.float32, jnp.bfloat16


def layer(
    pieces, chunks, x_hbm, k_hbm, v_hbm, ga_hbm, wq_hbm, wo_hbm, gm_hbm, wg_hbm, wu_hbm, wd_hbm, turn_hbm, y_ref,
    x_ref, ga_ref, gm_ref, turn_ref, wq_ref, wo_ref, wg_ref, wu_ref, wd_ref, k_ref, v_ref, w_ref, q_ref, seen_ref, a_ref, hidden_ref,
    *rest,
):
    counts = (len(pieces),) * 3 + (len(chunks),) * 4
    starts = [sum(counts[:n]) for n in range(len(counts) + 1)]
    own1, out1, in1, h_ref, own2, out2, in2 = (rest[a:b] for a, b in zip(starts, starts[1:]))
    sem, k_sem, v_sem, send_sem, recv_sem = rest[starts[-1] :]
    rows, d = x_ref.shape
    parts = h_ref[0].shape[0]
    part = d // parts
    me = lax.axis_index("tp")
    chip, core = me // 2, lax.rem(me, 2)

    def peer_of(ahead, other):
        return lax.rem(chip + ahead, parts // 2) * 2 + lax.rem(core + other, 2)

    barrier = pltpu.get_barrier_semaphore()
    for ahead, other in ORDER:
        pl.semaphore_signal(barrier, inc=1, device_id={"tp": peer_of(ahead, other)}, device_id_type=MESH)

    def load_at(i, src, dst):
        return pltpu.make_async_copy(src, dst, sem.at[i])

    first = [load_at(0, x_hbm, x_ref), load_at(1, ga_hbm, ga_ref), load_at(2, turn_hbm, turn_ref), load_at(3, wq_hbm, wq_ref)]
    second = [load_at(4, wo_hbm, wo_ref), load_at(5, gm_hbm, gm_ref)]
    third = [load_at(6, wg_hbm, wg_ref), load_at(7, wu_hbm, wu_ref), load_at(8, wd_hbm, wd_ref)]

    def load(hbm, ref, sem, step, half=None):
        slot = lax.rem(step, SLOTS)
        if half is None:
            return pltpu.make_async_copy(hbm.at[pl.ds(2 * step, 2)], ref.at[slot], sem.at[slot])
        return pltpu.make_async_copy(hbm.at[2 * step + half], ref.at[slot, half], sem.at[slot])

    def keys(step, half=None):
        return load(k_hbm, k_ref, k_sem, step, half)

    def values_of(step):
        return load(v_hbm, v_ref, v_sem, step)

    for c in first:
        c.start()
    keys(0, 0).start()

    with jax.named_scope("wait_x"):
        for c in first[:3]:
            c.wait()
        keys(0, 1).start()
        values_of(0).start()
        for c in first[3:]:
            c.wait()
    for n in range(2, DEPTH):
        (values_of if n % 2 else keys)(n // 2).start()
    wide = x_ref[...].astype(F32)
    scale = lax.rsqrt(jnp.mean(wide * wide, -1, keepdims=True) + 1e-6)
    a = (wide * scale * ga_ref[...].astype(F32).reshape(1, d)).astype(BF16)
    q = jnp.dot(a, wq_ref[...], preferred_element_type=F32).astype(BF16).astype(F32)
    lane = lax.broadcasted_iota(jnp.int32, q.shape, 1)
    width = q.shape[1]
    swapped = jnp.where(lane % HEAD < HEAD // 2, pltpu.roll(q, width - HEAD // 2, 1), pltpu.roll(q, HEAD // 2, 1))
    q_ref[...] = (q * turn_ref[0:1, :] + swapped * turn_ref[1:2, :]).astype(BF16).astype(F32)

    lane8 = lax.broadcasted_iota(jnp.int32, (STEP, width), 1) // HEAD
    row8 = lax.broadcasted_iota(jnp.int32, (STEP, width), 0)
    low = row8 < FOUR
    zero = jnp.zeros((STEP, width), F32)

    def everywhere(t):
        t = t + pltpu.roll(t, HEAD, 1)
        return t + pltpu.roll(t, 2 * HEAD, 1)

    def spread(rep):
        halves = []
        for j in range(2):
            z = everywhere(jnp.where(lane8 == 2 * j + row8 // FOUR, rep, zero))
            halves.append(jnp.where(lane8 == row8 % FOUR, z, zero))
        return jnp.concatenate(halves, 0).astype(BF16)

    def gathered(o):
        total = zero
        for j in range(2):
            z = everywhere(jnp.where(lane8 == row8 % FOUR, o[STEP * j : STEP * (j + 1)], zero))
            total = total + jnp.where(lane8 == 2 * j + row8 // FOUR, z, zero)
        return total + pltpu.roll(total, FOUR, 0)

    def scores(i, half, q8):
        turned8 = pltpu.roll(q8, FOUR, 0)
        rep = jnp.where(low, q8, turned8) if half == 0 else jnp.where(low, turned8, q8)
        s = jnp.dot(spread(rep), k_ref[lax.rem(i, SLOTS), half], preferred_element_type=F32)
        top = jnp.max(s, -1, keepdims=True)
        e = jnp.exp((s - top) * HEAD**-0.5)
        return (e * (1.0 / jnp.sum(e, -1, keepdims=True))).astype(BF16)

    def values(i, half, w):
        v = v_ref[lax.rem(i, SLOTS), half]
        return gathered(lax.dot_general(w, v, (((1,), (1,)), ((), ())), preferred_element_type=F32))

    def eight(i):
        return pl.ds(pl.multiple_of(i * STEP, STEP), STEP)

    def start_after(step, kind):
        later = step + (kind + DEPTH) // 2

        @pl.when(later < rows // STEP)
        def _():
            (values_of if (kind + DEPTH) % 2 else keys)(later).start()

    def weigh_all(i):
        with jax.named_scope("wait_k"):
            keys(i).wait()
        start_after(i, 0)
        q8 = q_ref[eight(i), :]
        for half in range(2):
            w_ref[half] = scores(i, half, q8)

    def attend_last(i):
        with jax.named_scope("wait_v"):
            values_of(i).wait()
        start_after(i, 1)
        seen_ref[eight(i), :] = jnp.where(low, values(i, 0, w_ref[0]), values(i, 1, w_ref[1]))

    def attend(i, _):
        weigh_all(i)
        attend_last(i)
        return 0

    n_pieces = len(pieces)

    def sent(e, src, dst, peer):
        return pltpu.make_async_remote_copy(
            src_ref=src, dst_ref=dst, send_sem=send_sem.at[e], recv_sem=recv_sem.at[e], device_id={"tp": peer}, device_id_type=MESH
        )

    def got(e, all_of):
        sent(e, all_of, all_of, peer_of(0, 1)).wait_recv()

    def all_but_one(ref):
        return ref.at[pl.ds(0, parts - 1)]

    def all_but_one_part(c):
        start, size, *_ = chunks[c]
        return y_ref.at[span(start, size), pl.ds(0, d - part)]

    def cols(p):
        return pl.ds(pl.multiple_of(p * part, part), part)

    def span(start, size):
        return pl.ds(start, size)

    def scatter(e, left, w_ref, own, out, into):
        for ahead, other in ORDER + HERE:
            p = peer_of(ahead, other)
            term = jnp.dot(left, w_ref[:, cols(p)], preferred_element_type=F32)
            if (ahead, other) == (0, 0):
                own[...] = term
            else:
                out[p] = term.astype(BF16)
        for ahead, other in ORDER:
            p = peer_of(ahead, other)
            sent(e, out.at[p], into.at[me], p).start()

    def summed(e, own, into, residual):
        got(e, all_but_one(into))
        total = own[...]
        for ahead, other in ORDER:
            total = total + into[peer_of(ahead, other)].astype(F32)
        return (residual + total).astype(BF16)

    chips = parts // 2
    half_d = d // 2
    mine = core * chips + chip

    def half_of(core_):
        return pl.ds(pl.multiple_of(core_ * half_d, half_d), half_d)

    def to_other(e, left, w_ref, own, out, into):
        out[0] = jnp.dot(left, w_ref[:, half_of(1 - core)], preferred_element_type=F32).astype(BF16)
        sent(e, out.at[0], into.at[parts], peer_of(0, 1)).start()
        own[...] = jnp.dot(left, w_ref[:, half_of(core)], preferred_element_type=F32)

    def to_all(e, own, out, into):
        got(e, into.at[parts])
        both = (own[...] + into[parts].astype(F32)).astype(BF16)
        out[1] = both
        into[mine] = both
        for ahead, other in ORDER:
            sent(e + 1, out.at[1], into.at[mine], peer_of(ahead, other)).start()

    def from_all(e, into):
        got(e + 1, all_but_one(into))

    def summed_all(into, residual, q):
        which, at = q * part // half_d, q * part % half_d
        total = into[which * chips, :, at : at + part].astype(F32)
        for p in range(1, chips):
            total = total + into[which * chips + p, :, at : at + part].astype(F32)
        return (residual + total).astype(BF16)

    def first_half(i):
        start, size, whole = pieces[i]
        (to_other if whole else scatter)(2 * i, seen_ref[span(start, size), :].astype(BF16), wo_ref, own1[i], out1[i], in1[i])

    def first_sum(i):
        start, size, whole = pieces[i]
        if whole:
            to_all(2 * i, own1[i], out1[i], in1[i])
            return
        at = h_ref[i].at[me]
        at[...] = summed(2 * i, own1[i], in1[i], x_ref[span(start, size), cols(me)].astype(F32))
        for ahead, other in ORDER:
            sent(2 * i + 1, at, at, peer_of(ahead, other)).start()

    def normed_first(c):
        start, size, _, members = chunks[c]
        for i in members:
            first, count, whole = pieces[i]
            if whole:
                from_all(2 * i, in1[i])
                for p in range(parts):
                    residual = x_ref[span(first, count), p * part : (p + 1) * part].astype(F32)
                    h_ref[c][p, first - start : first - start + count, :] = summed_all(in1[i], residual, p)
            else:
                got(2 * i + 1, all_but_one(h_ref[c]))
        squares = jnp.zeros((size, part), F32)
        for p in range(parts):
            wide = h_ref[c][p].astype(F32)
            squares = squares + wide * wide
        scale = lax.rsqrt(jnp.sum(squares, -1, keepdims=True) * (1.0 / d) + 1e-6)
        for p in range(parts):
            gain = gm_ref[p * part : (p + 1) * part].astype(F32).reshape(1, part)
            a_ref[0:size, p * part : (p + 1) * part] = (h_ref[c][p].astype(F32) * scale * gain).astype(BF16)

    def hidden(c, tiles=(0, 1)):
        size = chunks[c][1]
        tile = wg_ref.shape[1] // 2
        b = a_ref[0:size, :]
        for n in (t * tile for t in tiles):
            gate = jnp.dot(b, wg_ref[:, n : n + tile], preferred_element_type=F32)
            up = jnp.dot(b, wu_ref[:, n : n + tile], preferred_element_type=F32)
            hidden_ref[0:size, n : n + tile] = (gate * (1.0 / (1.0 + jnp.exp(-gate))) * up).astype(BF16)

    def exchange(c):
        return 2 * (n_pieces + c)

    def second_half(c):
        _, size, whole, _ = chunks[c]
        (to_other if whole else scatter)(exchange(c), hidden_ref[0:size, :], wd_ref, own2[c], out2[c], in2[c])

    def second_sum(c):
        start, size, whole, _ = chunks[c]
        if whole:
            to_all(exchange(c), own2[c], out2[c], in2[c])
            return
        at = y_ref.at[span(start, size), cols(me)]
        at[...] = summed(exchange(c), own2[c], in2[c], h_ref[c][me].astype(F32))
        for ahead, other in ORDER:
            sent(exchange(c) + 1, at, at, peer_of(ahead, other)).start()

    def last(c):
        start, size, whole, _ = chunks[c]
        if whole:
            from_all(exchange(c), in2[c])
            for p in range(parts):
                y_ref[span(start, size), p * part : (p + 1) * part] = summed_all(in2[c], h_ref[c][p].astype(F32), p)
            return
        got(exchange(c) + 1, all_but_one_part(c))

    def all_sent():
        def wait(e, all_of):
            sent(e, all_of, all_of, peer_of(0, 1)).wait_send()

        for i, (_, _, whole) in enumerate(pieces):
            wait(2 * i, out1[i].at[0] if whole else all_but_one(out1[i]))
            wait(2 * i + 1, all_but_one(in1[i] if whole else h_ref[i]))
        for c, (_, _, whole, _) in enumerate(chunks):
            wait(exchange(c), out2[c].at[0] if whole else all_but_one(out2[c]))
            wait(exchange(c) + 1, all_but_one(in2[c]) if whole else all_but_one_part(c))

    scope = jax.named_scope
    steps = rows // STEP
    ends = [(start + size) // STEP for start, size, _ in pieces]
    big, mid, late = range(3)
    lax.fori_loop(0, 2, attend, 0)
    for c in second:
        c.start()
    lax.fori_loop(2, ends[0], attend, 0)
    with scope("wait_wo"):
        for c in second:
            c.wait()
        pl.semaphore_wait(barrier, len(ORDER))
    with scope("first0"):
        first_half(0)
    lax.fori_loop(ends[0], ends[1], attend, 0)
    with scope("first1"):
        first_half(1)
    with scope("sum0"):
        first_sum(0)
    weigh_all(steps - 2)
    with scope("sum1"):
        first_sum(1)
    attend_last(steps - 2)
    for c in third:
        c.start()
    with scope("first2"):
        first_half(2)
    weigh_all(steps - 1)
    with scope("sum2"):
        first_sum(2)
    attend_last(steps - 1)
    with scope("first3"):
        first_half(3)
    with scope("norm0"):
        normed_first(big)
    with scope("wait_w"):
        for c in third[:2]:
            c.wait()
    with scope("hidden0"):
        hidden(big, (0,))
    with scope("sum3"):
        first_sum(3)
    with scope("hidden0"):
        hidden(big, (1,))
    third[2].wait()
    with scope("second0"):
        second_half(big)
    with scope("norm1"):
        normed_first(mid)
    with scope("hidden1"):
        hidden(mid)
    with scope("second1"):
        second_half(mid)
    with scope("norm2"):
        normed_first(late)
    with scope("hidden2"):
        hidden(late)
    with scope("ysum0"):
        second_sum(big)
    with scope("second2"):
        second_half(late)
    with scope("ysum2"):
        second_sum(late)
    with scope("ysum1"):
        second_sum(mid)
    with scope("last2"):
        last(late)
    with scope("last3"):
        last(big)
        last(mid)
    with scope("sent"):
        all_sent()


def solution(mesh):
    parts = mesh.shape["tp"]

    def step(x, k_cache, v_cache, gain_a, wq, wo, gain_m, w_gate, w_up, w_down):
        rows, d = x.shape
        seqs, places, kv_heads, head = k_cache.shape
        width = wq.shape[1]
        part = d // parts
        k, v = (jnp.transpose(t, (0, 2, 3, 1)).reshape(seqs // FOUR, FOUR * kv_heads * head, places) for t in (k_cache, v_cache))
        half = head // 2
        angle = np.float32(places - 1) * np.float32(THETA) ** (-np.arange(half, dtype=np.float32) / np.float32(half))
        angle = angle.astype(np.float32)
        cos, sin = np.cos(angle).astype(np.float32), np.sin(angle).astype(np.float32)
        turn = np.stack([np.tile(cos, width // half), np.tile(np.concatenate([-sin, sin]), width // head)])
        pieces = ((0, rows - 4 * STEP, False), (rows - 4 * STEP, 2 * STEP, True), (rows - 2 * STEP, STEP, True), (rows - STEP, STEP, True))
        chunks = ((0, rows - 4 * STEP, False, (0,)), (rows - 4 * STEP, 3 * STEP, False, (1, 2)), (rows - STEP, STEP, True, (3,)))
        sizes = [size for _, size, *_ in chunks]
        scratch = [
            pltpu.VMEM(x.shape, BF16),
            pltpu.VMEM((d,), BF16),
            pltpu.VMEM((d,), BF16),
            pltpu.VMEM(turn.shape, F32),
            *[pltpu.VMEM(w.shape, BF16) for w in (wq, wo, w_gate, w_up, w_down)],
            pltpu.VMEM((SLOTS, 2) + k.shape[1:], BF16),
            pltpu.VMEM((SLOTS, 2) + v.shape[1:], BF16),
            pltpu.VMEM((2, FOUR * width // head, places), BF16),
            pltpu.VMEM((rows, width), F32),
            pltpu.VMEM((rows, width), F32),
            pltpu.VMEM((max(sizes), d), BF16),
            pltpu.VMEM((max(sizes), w_gate.shape[1]), BF16),
        ]

        def buffers(sums):
            each = [(size, whole) for _, size, whole, *_ in sums]
            return (
                [pltpu.VMEM((size, d // 2 if whole else part), F32) for size, whole in each]
                + [pltpu.VMEM((2, size, d // 2) if whole else (parts, size, part), BF16) for size, whole in each]
                + [pltpu.VMEM((parts + 1, size, d // 2) if whole else (parts, size, part), BF16) for size, whole in each]
            )

        scratch += buffers(pieces) + [pltpu.VMEM((parts, size, part), BF16) for size in sizes] + buffers(chunks)
        scratch += [
            pltpu.SemaphoreType.DMA((9,)),
            pltpu.SemaphoreType.DMA((SLOTS,)),
            pltpu.SemaphoreType.DMA((SLOTS,)),
            pltpu.SemaphoreType.DMA((2 * (len(pieces) + len(chunks)),)),
            pltpu.SemaphoreType.DMA((2 * (len(pieces) + len(chunks)),)),
        ]
        return pl.pallas_call(
            functools.partial(layer, pieces, chunks),
            out_shape=pltpu.VMEM(x.shape, BF16),
            in_specs=[pl.BlockSpec(memory_space=pl.ANY)] * 11,
            out_specs=pl.BlockSpec(memory_space=pltpu.VMEM),
            scratch_shapes=scratch,
            compiler_params=pltpu.CompilerParams(collective_id=0, has_side_effects=True, vmem_limit_bytes=60 * 1024 * 1024),
            name="layer",
        )(x, k, v, gain_a, wq, wo, gain_m, w_gate, w_up, w_down, jnp.asarray(turn))

    states, cache, columns, rows_of = P("dp", None), P("dp", None, "tp", None), P(None, "tp"), P("tp", None)
    return jax.shard_map(
        step,
        mesh=mesh,
        in_specs=(states, cache, cache, P(None), columns, rows_of, P(None), columns, columns, rows_of),
        out_specs=states,
        check_vma=False,
    )
```
